256 devices in a mesh: gx: 2 (over x_lo), gy: 8 (over x_hi, y), gz: 16 (over z, core).
Axes of the slice: x: 4 (x_hi: 2, x_lo: 2; x = x_hi * 2 + x_lo), y: 4, z: 8, core: 2. Of those that a mesh axis runs over, the one named last changes fastest.
Arguments:
- volume: bfloat16 [32, 64, 64, 256], P(None, 'gx', 'gy', 'gz'), may hold values from -6 to 6
- weight_a: bfloat16 [3, 3, 3, 32, 64], replicated, may hold values from -0.21875 to 0.21875
- bias_a: float32 [64], replicated, may hold values from -3 to 3
- weight_b: bfloat16 [3, 3, 3, 64, 128], replicated, may hold values from -0.15625 to 0.15625
- bias_b: float32 [128], replicated, may hold values from -3 to 3
- cotangent: bfloat16 [128, 32, 32, 128], P(None, ('gx', 'gz'), 'gy'), may hold values from -24 to 24
Outputs:
- features: bfloat16 [128, 32, 32, 128], P(None, ('gx', 'gz'), 'gy')
- grad_input: bfloat16 [32, 64, 64, 256], P(None, 'gx', 'gy', 'gz')
- grad_weight_a: float32 [3, 3, 3, 32, 64], replicated
- grad_bias_a: float32 [64], replicated
- grad_weight_b: float32 [3, 3, 3, 64, 128], replicated
- grad_bias_b: float32 [128], replicated
The draws below stay inside these ranges and needn't reach their ends.
All inputs are finite; a program needn't handle non-finite values.
Results may differ from the reference program's by a relative error of at most 0.012.
Values may be sent and summed in bfloat16 or wider, within the bound.
A program may use at most 128 MiB of HBM per device.

```python
import math
import jax
import jax.numpy as jnp
from jax import lax

C1 = 32
C2 = 64
C3 = 128
NX = 64
NY = 64
NZ = 256


def level_of(key, dims, shards, least, top_value):
    def one(axis_at, blocks):
        steps = jax.random.uniform(jax.random.fold_in(jax.random.fold_in(key, 6), axis_at), (blocks,), jnp.float32, least / len(shards), top_value / len(shards))
        return jnp.repeat(jnp.exp(steps), dims[axis_at] // blocks).reshape((-1,) + (1,) * (len(dims) - axis_at - 1))

    level = one(*shards[0])
    for cut in shards[1:]:
        level = level * one(*cut)
    return level


def centred(own_key, shape, deviation, limit, cuts=(), dtype=jnp.bfloat16):
    entries = deviation * jax.random.normal(own_key, shape, jnp.float32)
    if cuts:
        entries = entries * level_of(own_key, shape, cuts, -0.22, 0.18)
    return jnp.clip(entries, -limit, limit).astype(dtype)


def setup_inputs(seed: int = 0) -> dict:
    seeds = jax.random.split(jax.random.key(seed), 7)
    return {
        "volume": centred(seeds[0], (C1, NX, NY, NZ), 1.0, 6.0, ((1, 2), (2, 8), (3, 16))),
        "weight_a": centred(seeds[1], (3, 3, 3, C1, C2), (27 * C1) ** -0.5, 0.21875),
        "bias_a": centred(seeds[2], (C2,), 0.5, 3.0, (), jnp.float32),
        "weight_b": centred(seeds[3], (3, 3, 3, C2, C3), (27 * C2) ** -0.5, 0.15625),
        "bias_b": centred(seeds[4], (C3,), 0.5, 3.0, (), jnp.float32),
        "cotangent": centred(seeds[5], (C3, NX // 2, NY // 2, NZ // 2), 4.0, 24.0, ((1, 32), (2, 8))),
    }


def activate(value):
    return value * jax.nn.sigmoid(value)

def slope_of(value):
    sigma = jax.nn.sigmoid(value)
    return sigma + value * sigma * (1.0 - sigma)

def conv_valid(padded, weight):
    result = lax.conv_general_dilated(padded[None], weight, (1, 1, 1), 'VALID', dimension_numbers=('NCDHW', 'DHWIO', 'NCDHW'), preferred_element_type=jnp.float32)
    return result[0]

def flipped(weight):
    return jnp.transpose(weight[::-1, ::-1, ::-1], (0, 1, 2, 4, 3))

def pad_all(field):
    return jnp.pad(field, ((0, 0), (1, 1), (1, 1), (1, 1)))

def average_pool(field):
    shape = field.shape
    split = field.reshape(shape[0], shape[1] // 2, 2, shape[2] // 2, 2, shape[3] // 2, 2)
    return lax.optimization_barrier(jnp.sum(split, axis=(2, 4, 6))) * 0.125

def spread_back(field):
    shape = field.shape
    larger = jnp.broadcast_to(field[:, :, None, :, None, :, None], (shape[0], shape[1], 2, shape[2], 2, shape[3], 2))
    return larger.reshape(shape[0], 2 * shape[1], 2 * shape[2], 2 * shape[3])

def weight_terms(padded, grad):
    width_in = padded.shape[0]
    width_out = grad.shape[0]
    extent = grad.shape[1:]
    flattened = grad.reshape(width_out, extent[0] * extent[1] * extent[2])
    products = []
    for first in range(3):
        for second in range(3):
            for third in range(3):
                window = padded[:, first:first + extent[0], second:second + extent[1], third:third + extent[2]]
                window = window.reshape(width_in, extent[0] * extent[1] * extent[2])
                products.append(lax.dot_general(window, flattened, (((1,), (1,)), ((), ())), preferred_element_type=jnp.float32))
    return jnp.stack(products).reshape(3, 3, 3, width_in, width_out)

def reference(volume, weight_a, bias_a, weight_b, bias_b, cotangent):
    scale_a = 1.0 / math.sqrt(NX * NY * NZ)
    scale_b = 1.0 / math.sqrt(NX * NY * NZ // 8)
    padded_a = pad_all(volume)
    before_a = conv_valid(padded_a, weight_a) + bias_a[:, None, None, None]
    pooled = average_pool(activate(before_a)).astype(jnp.bfloat16)
    padded_b = pad_all(pooled)
    before_b = conv_valid(padded_b, weight_b) + bias_b[:, None, None, None]
    features = activate(before_b).astype(jnp.bfloat16)
    grad_b = (cotangent.astype(jnp.float32) * slope_of(before_b)).astype(jnp.bfloat16)
    grad_weight_b = weight_terms(padded_b, grad_b) * scale_b
    grad_bias_b = lax.optimization_barrier(jnp.sum(grad_b.astype(jnp.float32), axis=(1, 2, 3))) * scale_b
    grad_pooled = conv_valid(pad_all(grad_b), flipped(weight_b)).astype(jnp.bfloat16)
    grad_a = (spread_back(grad_pooled.astype(jnp.float32)) * 0.125 * slope_of(before_a)).astype(jnp.bfloat16)
    grad_weight_a = weight_terms(padded_a, grad_a) * scale_a
    grad_bias_a = lax.optimization_barrier(jnp.sum(grad_a.astype(jnp.float32), axis=(1, 2, 3))) * scale_a
    grad_input = conv_valid(pad_all(grad_a), flipped(weight_a)).astype(jnp.bfloat16)
    return (features, grad_input, grad_weight_a, grad_bias_a, grad_weight_b, grad_bias_b)
```

```python
import math

import jax
import jax.numpy as jnp
from jax import lax
from jax.experimental import pallas as pl
from jax.experimental.pallas import tpu as pltpu
from jax.sharding import PartitionSpec as P

F32 = jnp.float32
BF16 = jnp.bfloat16
MESH = pl.DeviceIdType.MESH
GX, GY, GZ, GROUP = 2, 8, 16, 32
PITCH = 24
CHUNK_A, CHUNK_B = 16, 64


class Halo:
    def __init__(self, length, sides):
        self.length, self.sides = length, sides
        self.messages, self.staged, self.stage_rows, self.rows = [], {}, 0, 0
        for dx in (0, 1):
            for dy in (-1, 0, 1):
                for dz in (-1, 0, 1):
                    if not (dx or dy or dz):
                        continue
                    blocks, count = [], 0
                    for q, side in enumerate(sides):
                        if dy and dy not in side:
                            continue
                        if dx:
                            rows = 16 if dy else 32
                        elif dy:
                            rows = length if dz else 8 * length
                        else:
                            rows = 4 * length
                        blocks.append((q, count, rows))
                        count += rows
                    key = (dx, dy, 0 if dx else dz)
                    if key not in self.staged:
                        self.staged[key] = (self.stage_rows, blocks)
                        self.stage_rows += count
                    self.messages.append((dx, dy, dz, key, count, self.rows, blocks))
                    self.rows += count

    def grid(self, ref):
        return ref.reshape(self.length + 2, 6, PITCH, 128)

    def send(self, at, grids, stage, landed, send_sem, recv_sem):
        n = self.length
        gx, gy, gz = at
        edge = n - gx * (n - 1)
        for (dx, dy, dz), (start, blocks) in self.staged.items():
            ys = 4 if dy < 0 else 1
            zs = 15 if dz < 0 else 8
            for q, offset, rows in blocks:
                flat, grid = grids[q], self.grid(grids[q])
                row = start + offset
                if dx:
                    if dy:
                        tile = grid[edge, ys, 8:16, :]
                        value = jnp.concatenate([tile, tile], axis=0)
                    else:
                        value = grid[edge, 1:5, 8:16, :].reshape(32, 128)
                    stage[row : row + rows, :] = value.astype(BF16)
                elif dz == 0:
                    value = grid[1 : n + 1, ys, 8:16, :].reshape(8 * n, 128)
                    stage[row : row + rows, :] = value.astype(BF16)
                else:
                    for k, y in enumerate((ys,) if dy else (1, 2, 3, 4)):
                        value = flat[pl.ds((6 + y) * PITCH + zs, n, stride=6 * PITCH), :]
                        stage[row + k * n : row + (k + 1) * n, :] = value.astype(BF16)
        for dx, dy, dz, key, count, row, _ in self.messages:
            start = self.staged[key][0]
            target = (
                1 - gx if dx else gx,
                lax.rem(gy + (GY - dy), GY) if dy else gy,
                lax.rem(gz + (GZ - dz), GZ) if dz else gz,
            )
            pltpu.make_async_remote_copy(
                src_ref=stage.at[start : start + count],
                dst_ref=landed.at[row : row + count],
                send_sem=send_sem,
                recv_sem=recv_sem,
                device_id=target,
                device_id_type=MESH,
            ).start()

    def receive(self, at, grids, landed, recv_sem):
        n = self.length
        gx, gy, gz = at
        far = (n + 1) * (1 - gx)
        for grid in grids:
            self.grid(grid)[(n + 1) * gx, :, :, :] = jnp.zeros((6, PITCH, 128), F32)
        pltpu.make_async_copy(landed, landed, recv_sem).wait()
        inside_y = {-1: gy > 0, 0: None, 1: gy < GY - 1}
        inside_z = {-1: gz > 0, 0: None, 1: gz < GZ - 1}
        for dx, dy, dz, _, _, start, blocks in self.messages:
            yd = 0 if dy < 0 else 5
            zd = 7 if dz < 0 else 16
            tile = 8 * (dz + 1)
            keep = [c for c in (inside_y[dy], inside_z[dz]) if c is not None]
            for q, offset, rows in blocks:
                flat, grid = grids[q], self.grid(grids[q])
                row = start + offset

                def take(first, size):
                    value = landed[first : first + size, :].astype(F32)
                    for c in keep:
                        value = jnp.where(c, value, 0.0)
                    return value

                if dx and dy:
                    grid[far, yd, tile : tile + 8, :] = take(row, 16)[:8]
                elif dx:
                    grid[far, 1:5, tile : tile + 8, :] = take(row, 32).reshape(4, 8, 128)
                elif dz == 0:
                    grid[1 : n + 1, yd, 8:16, :] = take(row, 8 * n).reshape(n, 8, 128)
                else:
                    for k, y in enumerate((yd,) if dy else (1, 2, 3, 4)):
                        flat[pl.ds((6 + y) * PITCH + zd, n, stride=6 * PITCH), :] = take(row + k * n, n)


HALO_VOLUME = Halo(32, ((-1, 1),))
HALO_COARSE = Halo(16, ((-1, 1),))
HALO_GRAD_A = Halo(32, ((1,), (-1,)))


def row_block(jy, jz):
    ty, py = (0, jy - 1) if jy in (1, 2) else (1, 1 if jy == 0 else 0)
    tz, pz = (0, jz - 1) if jz in (1, 2) else (1, 1 if jz == 0 else 0)
    return (ty * 2 + tz) * 4 + py * 2 + pz


def fine_offset(shifted, parity):
    if not shifted:
        return 1 + parity
    return 0 if parity else 3


def lanes_at_least(shape, width, period=None):
    lane = lax.broadcasted_iota(jnp.int32, shape, len(shape) - 1)
    if period:
        lane = lax.rem(lane, period)
    return lane >= width


class Sum:
    def __init__(self, at, chunk, send, got, mids, out, sems):
        gx, gy, gz = at
        self.gx, self.gy, self.gz = at
        self.z, self.core = lax.div(gz, 2), lax.rem(gz, 2)
        self.rank = (gx * GY + gy) * 2 + self.core
        self.chunk, self.parts, self.got, self.mids, self.out, self.sems = chunk, send, got, mids, out, sems

    def plane_peer(self, rank):
        return (lax.div(rank, 16), lax.rem(lax.div(rank, 2), GY), self.z * 2 + lax.rem(rank, 2))

    def rows(self, k):
        return pl.ds(pl.multiple_of(k * self.chunk, self.chunk), self.chunk)

    def scatter(self):
        def issue(r, _):
            peer = lax.rem(self.rank + r, GROUP)
            pltpu.make_async_remote_copy(
                src_ref=self.parts.at[self.rows(peer)],
                dst_ref=self.got.at[self.rows(r - 1)],
                send_sem=self.sems.at[0],
                recv_sem=self.sems.at[1],
                device_id=self.plane_peer(peer),
                device_id_type=MESH,
            ).start()
            return 0

        lax.fori_loop(1, GROUP, issue, 0)

    def exchange(self):
        pltpu.make_async_copy(self.got, self.got, self.sems.at[1]).wait()

        def add(r, total):
            return total + self.got[self.rows(r), :].astype(F32)

        total = lax.fori_loop(0, GROUP - 1, add, self.parts[self.rows(self.rank), :].astype(F32))
        self.mids[self.rows(self.z), :] = total.astype(BF16)

        def issue(r, _):
            peer = lax.rem(self.z + r, 8)
            pltpu.make_async_remote_copy(
                src_ref=self.mids.at[self.rows(self.z)],
                dst_ref=self.mids.at[self.rows(self.z)],
                send_sem=self.sems.at[2],
                recv_sem=self.sems.at[3],
                device_id=(self.gx, self.gy, peer * 2 + self.core),
                device_id_type=MESH,
            ).start()
            return 0

        lax.fori_loop(1, 8, issue, 0)

    def gather(self):
        seven = self.mids.at[0 : 7 * self.chunk]
        pltpu.make_async_copy(seven, seven, self.sems.at[3]).wait()
        total = self.mids[0 : self.chunk, :].astype(F32)
        for k in range(1, 8):
            total = total + self.mids[k * self.chunk : (k + 1) * self.chunk, :].astype(F32)
        self.out[self.rows(self.rank), :] = total.astype(BF16)

        def issue(r, _):
            peer = lax.rem(self.rank + r, GROUP)
            pltpu.make_async_remote_copy(
                src_ref=self.out.at[self.rows(self.rank)],
                dst_ref=self.out.at[self.rows(self.rank)],
                send_sem=self.sems.at[4],
                recv_sem=self.sems.at[5],
                device_id=self.plane_peer(peer),
                device_id_type=MESH,
            ).start()
            return 0

        lax.fori_loop(1, GROUP, issue, 0)

    def finish(self):
        pltpu.make_async_copy(self.got, self.got, self.sems.at[5]).wait()

    def drain(self):
        seven = self.mids.at[0 : 7 * self.chunk]
        pltpu.make_async_copy(self.got, self.got, self.sems.at[0]).wait()
        pltpu.make_async_copy(seven, seven, self.sems.at[2]).wait()
        pltpu.make_async_copy(self.got, self.got, self.sems.at[4]).wait()


def kernel(
    scale_a, scale_b,
    volume, weight_a, bias_a, weight_b, bias_b, cot,
    features, grad_input, dwa, dba, dwb, dbb,
    fine, coarse, grad_c, fine_0, fine_1,
    lhs_a, lhs_b, lhs_c, lhs_f,
    pairs, mat_a, mat_b, mat_bt, mat_at,
    slope_a, feat, cot_here, gb, ga, dw,
    stage_v, land_v, stage_p, land_p, stage_g, land_g, stage_f, land_f,
    send_a, got_a, mid_a, out_a, send_b, got_b, mid_b, out_b,
    halo_sems, slab_sems, sems_a, sems_b,
):
    gx, gy, gz = lax.axis_index("gx"), lax.axis_index("gy"), lax.axis_index("gz")
    at = (gx, gy, gz)
    core = lax.rem(gz, 2)
    zero = jnp.zeros((32, 64), F32)

    barrier = pltpu.get_barrier_semaphore()

    def signal(target):
        pl.semaphore_signal(barrier, inc=1, device_id=target, device_id_type=MESH)

    def along_z(r, _):
        signal((gx, gy, lax.rem(gz + r, GZ)))
        return 0

    def in_plane(r, _):
        cell = lax.rem(gx * GY + gy + r, 16)
        for c in range(2):
            signal((lax.div(cell, GY), lax.rem(cell, GY), gz - core + c))
        return 0

    lax.fori_loop(1, GZ, along_z, 0)
    lax.fori_loop(1, 16, in_plane, 0)
    side = lax.rem(gz + GZ - 1 + 2 * core, GZ)
    for dx in (0, 1):
        for dy in (-1, 0, 1):
            if dx or dy:
                signal((1 - gx if dx else gx, lax.rem(gy + GY + dy, GY) if dy else gy, side))

    grid_v = HALO_VOLUME.grid(fine)

    def load_volume(x, _):
        rows = volume[pl.ds(pl.multiple_of(x * 32, 32), 32), :].astype(F32)
        grid_v[x + 1, 1:5, 8:16, :] = rows.reshape(4, 8, 128)
        return 0

    lax.fori_loop(0, 32, load_volume, 0)
    pl.semaphore_wait(barrier, 50)
    HALO_VOLUME.send(at, (fine,), stage_v, land_v, halo_sems.at[0], halo_sems.at[1])

    def slab_rows(k):
        return pl.ds(pl.multiple_of(k * 32, 32), 32)

    def send_cot(r, _):
        peer = lax.rem(gz + r, GZ)
        pltpu.make_async_remote_copy(
            src_ref=cot.at[slab_rows(peer)],
            dst_ref=cot_here.at[slab_rows(gz)],
            send_sem=slab_sems.at[0],
            recv_sem=slab_sems.at[1],
            device_id=(gx, gy, peer),
            device_id_type=MESH,
        ).start()
        return 0

    lax.fori_loop(1, GZ, send_cot, 0)
    cot_here[slab_rows(gz), :] = cot[slab_rows(gz), :]

    def make_pairs(k, _):
        w0 = weight_a[3 * k].astype(F32)
        w1 = weight_a[3 * k + 1].astype(F32)
        w2 = weight_a[3 * k + 2].astype(F32)
        for j, (left, right) in enumerate(((w0, zero), (w1, w0), (w2, w1), (zero, w2))):
            rows = pl.ds(pl.multiple_of(k * 128 + j * 32, 32), 32)
            pairs[rows, :] = jnp.concatenate([left, right], axis=1).astype(BF16)
        return 0

    lax.fori_loop(0, 9, make_pairs, 0)

    def pair(kxy, j):
        return pairs[pl.ds(pl.multiple_of(kxy * 128 + j * 32, 32), 32), :]

    def make_mats(kx, _):
        for t in range(4):
            ty, tz = t // 2, t % 2
            for py in range(2):
                jy = fine_offset(ty, py)
                for out_y in range(2):
                    ky = jy - out_y
                    inside = 0 <= ky <= 2
                    for pz in range(2):
                        jz = fine_offset(tz, pz)
                        row = kx * 512 + t * 128 + py * 64 + pz * 32
                        value = pair(kx * 3 + ky, jz) if inside else jnp.zeros((32, 128), BF16)
                        mat_a[pl.ds(pl.multiple_of(row, 32), 32), out_y * 128 : out_y * 128 + 128] = value
                    for out_z in range(2):
                        j = (3, 0)[out_z] if tz else (1, 2)[out_z]
                        row = kx * 128 + (out_y * 2 + out_z) * 32
                        value = (
                            pair((2 - kx) * 3 + 2 - ky, j) if inside else jnp.zeros((32, 128), BF16)
                        )
                        lane = (t * 2 + py) * 128
                        mat_at[pl.ds(pl.multiple_of(row, 32), 32), lane : lane + 128] = value
        parts = [(0, 0), (0, 2), (1, 0), (1, 2), (2, 0), (2, 2), (0, 1), (1, 1), (2, 1)]
        for j, (ky, kz) in enumerate(parts):
            row = kx * 640 + j * 64
            mat_b[pl.ds(pl.multiple_of(row, 64), 64), :] = weight_b[kx * 9 + ky * 3 + kz]
        mat_b[pl.ds(pl.multiple_of(kx * 640 + 576, 64), 64), :] = jnp.zeros((64, 128), BF16)
        for ky in range(3):
            for kz in range(3):
                lane = (ky * 3 + kz) * 128
                value = weight_b[(2 - kx) * 9 + (2 - ky) * 3 + 2 - kz]
                for c in range(2):
                    row = pl.ds(pl.multiple_of(kx * 128 + c * 64, 64), 64)
                    mat_bt[row, lane : lane + 128] = value
        return 0

    lax.fori_loop(0, 3, make_mats, 0)

    HALO_VOLUME.receive(at, (fine,), land_v, halo_sems.at[1])
    odd_z = lanes_at_least((6, 8, 128), 32, 64)
    odd_y = lanes_at_least((4, 8, 128), 64)
    upper = lanes_at_least((6, 8, 128), 64)

    def put(lhs, x, tile, value):
        rows = pl.ds(pl.multiple_of(x * 32, 32), 32)
        lhs[rows, tile * 128 : tile * 128 + 128] = value.reshape(32, 128).astype(BF16)

    def build_a(x, _):
        here = grid_v[x, :, 8:16, :]
        beside = jnp.where(odd_z, grid_v[x, :, 7:15, :], grid_v[x, :, 9:17, :])
        put(lhs_a, x, 0, here[1:5])
        put(lhs_a, x, 1, beside[1:5])
        put(lhs_a, x, 2, jnp.where(odd_y, here[0:4], here[2:6]))
        put(lhs_a, x, 3, jnp.where(odd_y, beside[0:4], beside[2:6]))
        return 0

    lax.fori_loop(0, 34, build_a, 0)
    grid_p = HALO_COARSE.grid(coarse)
    bias_a4 = jnp.concatenate([bias_a[...]] * 4, axis=1)

    def conv_a(i, _):
        row = i * 256
        value = bias_a4
        for kx in range(3):
            rows = pl.ds(pl.multiple_of(row + kx * 32, 32), 256)
            value = value + jnp.dot(
                lhs_a[rows, :], mat_a[kx * 512 : kx * 512 + 512, :], preferred_element_type=F32
            )
        sigma = jax.nn.sigmoid(value)
        active = value * sigma
        slope_a[pl.ds(pl.multiple_of(row, 256), 256), :] = sigma + active * (1.0 - sigma)
        total = active.reshape(4, 2, 32, 256)
        total = (total[:, 0] + total[:, 1]).reshape(128, 256)
        total = total[:, :128] + total[:, 128:]
        total = (total + pltpu.roll(total, 64, 1)) * 0.125
        total = total.astype(BF16).astype(F32)
        grid_p[pl.ds(1 + i * 4, 4), 1:5, 8:16, :] = total.reshape(4, 4, 8, 128)
        return 0

    lax.fori_loop(0, 4, conv_a, 0)
    HALO_COARSE.send(at, (coarse,), stage_p, land_p, halo_sems.at[2], halo_sems.at[3])

    send_b[1728:2048, :] = jnp.zeros((320, 128), BF16)
    send_a[464:512, :] = jnp.zeros((48, 128), BF16)
    HALO_COARSE.receive(at, (coarse,), land_p, halo_sems.at[3])

    def build_b(x, _):
        here = grid_p[x, :, 8:16, :]
        beside = jnp.where(upper, grid_p[x, :, 9:17, :], grid_p[x, :, 7:15, :])
        for ky in range(3):
            put(lhs_b, x, ky, beside[ky : ky + 4])
        put(lhs_b, x, 3, jnp.where(upper[:4], here[1:5], here[0:4]))
        put(lhs_b, x, 4, jnp.where(upper[:4], 0.0, here[2:6]))
        return 0

    lax.fori_loop(0, 18, build_b, 0)
    fifteen = cot_here.at[0:480]
    pltpu.make_async_copy(fifteen, fifteen, slab_sems.at[1]).wait()
    grid_g = HALO_COARSE.grid(grad_c)

    def conv_b(i, _):
        row = i * 256
        value = bias_b[...]
        for kx in range(3):
            rows = pl.ds(pl.multiple_of(row + kx * 32, 32), 256)
            value = value + jnp.dot(
                lhs_b[rows, :], mat_b[kx * 640 : kx * 640 + 640, :], preferred_element_type=F32
            )
        sigma = jax.nn.sigmoid(value)
        active = value * sigma
        rows = pl.ds(pl.multiple_of(row, 256), 256)
        feat[rows, :] = active.astype(BF16)
        grad = (cot_here[rows, :].astype(F32) * (sigma + active * (1.0 - sigma))).astype(BF16)
        gb[rows, :] = grad
        grid_g[pl.ds(1 + i * 8, 8), 1:5, 8:16, :] = grad.astype(F32).reshape(8, 4, 8, 128)
        return 0

    lax.fori_loop(0, 2, conv_b, 0)
    HALO_COARSE.send(at, (grad_c,), stage_g, land_g, halo_sems.at[4], halo_sems.at[5])

    def send_features(r, _):
        peer = lax.rem(gz + r, GZ)
        pltpu.make_async_remote_copy(
            src_ref=feat.at[slab_rows(peer)],
            dst_ref=features.at[slab_rows(gz)],
            send_sem=slab_sems.at[2],
            recv_sem=slab_sems.at[3],
            device_id=(gx, gy, peer),
            device_id_type=MESH,
        ).start()
        return 0

    lax.fori_loop(1, GZ, send_features, 0)
    features[slab_rows(gz), :] = feat[slab_rows(gz), :]

    across = (((0,), (0,)), ((), ()))
    along = (((1,), (1,)), ((), ()))

    def grad_of_b(kx, _):
        rows = pl.ds(pl.multiple_of(kx * 32, 32), 512)
        for t in range(5):
            value = lax.dot_general(
                lhs_b[rows, t * 128 : t * 128 + 128], gb[...], across, preferred_element_type=F32
            ).astype(BF16)
            places = (t * 3, t * 3 + 2) if t < 3 else ((1, 4) if t == 3 else (7,))
            for half, k in enumerate(places):
                row = pl.ds(pl.multiple_of((kx * 9 + k) * 64, 64), 64)
                send_b[row, :] = value[half * 64 : half * 64 + 64]
        return 0

    lax.fori_loop(0, 3, grad_of_b, 0)
    bias_sum = jnp.sum(gb[...].astype(F32), axis=0, keepdims=True)
    send_b[1728:1744, :] = jnp.broadcast_to(bias_sum, (16, 128)).astype(BF16)
    sum_b = Sum(at, CHUNK_B, send_b, got_b, mid_b, out_b, sems_b)
    sum_b.scatter()

    HALO_COARSE.receive(at, (grad_c,), land_g, halo_sems.at[5])

    def build_c(x, _):
        for kz in range(3):
            value = grid_g[x, :, 7 + kz : 15 + kz, :]
            for ky in range(3):
                put(lhs_c, x, ky * 3 + kz, value[ky : ky + 4])
        return 0

    lax.fori_loop(0, 18, build_c, 0)
    grids_f = [HALO_GRAD_A.grid(fine_0), HALO_GRAD_A.grid(fine_1)]

    def back_b(i, _):
        value = jnp.zeros((128, 128), F32)
        for kx in range(3):
            rows = pl.ds(pl.multiple_of(i * 128 + kx * 32, 32), 128)
            value = value + lax.dot_general(
                lhs_c[rows, :], mat_bt[kx * 128 : kx * 128 + 128, :], along, preferred_element_type=F32
            )
        value = value.astype(BF16).astype(F32) * 0.125
        value = jnp.broadcast_to(value.reshape(4, 1, 32, 128), (4, 2, 32, 128)).reshape(256, 128)
        rows = pl.ds(pl.multiple_of(i * 256, 256), 256)
        for py in range(2):
            lanes = slice(py * 128, py * 128 + 128)
            grad = (value * slope_a[rows, lanes]).astype(BF16)
            ga[rows, lanes] = grad
            grids_f[py][pl.ds(1 + i * 8, 8), 1:5, 8:16, :] = grad.astype(F32).reshape(8, 4, 8, 128)
        return 0

    lax.fori_loop(0, 4, back_b, 0)
    HALO_GRAD_A.send(at, (fine_0, fine_1), stage_f, land_f, halo_sems.at[6], halo_sems.at[7])

    def grad_of_a(kx, _):
        rows = pl.ds(pl.multiple_of(kx * 32, 32), 1024)
        for t in range(4):
            row = pl.ds(pl.multiple_of(kx * 512 + t * 128, 128), 128)
            dw[row, :] = lax.dot_general(
                lhs_a[rows, t * 128 : t * 128 + 128], ga[...], across, preferred_element_type=F32
            )
        return 0

    lax.fori_loop(0, 3, grad_of_a, 0)
    high = lanes_at_least((32, 128), 64)

    def block_sum(kx, ky, jz):
        total = None
        for out_y in range(2):
            row = kx * 512 + row_block(ky + out_y, jz) * 32
            part = dw[row : row + 32, out_y * 128 : out_y * 128 + 128]
            total = part if total is None else total + part
        return total

    for k in range(14):
        kx, ky, kz = k // 9, k // 3 % 3, k % 3
        value = block_sum(kx, ky, kz) + pltpu.roll(block_sum(kx, ky, kz + 1), 64, 1)
        other = jnp.zeros((32, 128), F32)
        if k + 14 < 27:
            kx, ky, kz = (k + 14) // 9, (k + 14) // 3 % 3, (k + 14) % 3
            other = pltpu.roll(block_sum(kx, ky, kz), 64, 1) + block_sum(kx, ky, kz + 1)
        send_a[k * 32 : k * 32 + 32, :] = jnp.where(high, other, value).astype(BF16)
    bias_sum = jnp.sum(ga[...].astype(F32), axis=0, keepdims=True)
    bias_sum = jnp.broadcast_to(bias_sum[:, :128] + bias_sum[:, 128:], (16, 128))
    send_a[448:464, :] = (bias_sum + pltpu.roll(bias_sum, 64, 1)).astype(BF16)
    sum_a = Sum(at, CHUNK_A, send_a, got_a, mid_a, out_a, sems_a)
    sum_a.scatter()
    sum_b.exchange()

    HALO_GRAD_A.receive(at, (fine_0, fine_1), land_f, halo_sems.at[7])

    def build_f(x, _):
        for q, grid in enumerate(grids_f):
            low = 1 - q
            here = grid[x, low : low + 5, 8:16, :]
            beside = jnp.where(
                upper[:5], grid[x, low : low + 5, 7:15, :], grid[x, low : low + 5, 9:17, :]
            )
            near, far = (slice(1, 5), slice(0, 4)) if q else (slice(0, 4), slice(1, 5))
            put(lhs_f, x, q, here[near])
            put(lhs_f, x, 2 + q, beside[near])
            put(lhs_f, x, 4 + q, here[far])
            put(lhs_f, x, 6 + q, beside[far])
        return 0

    lax.fori_loop(0, 34, build_f, 0)
    sum_a.exchange()

    def back_a(i, _):
        value = jnp.zeros((256, 128), F32)
        for kx in range(3):
            rows = pl.ds(pl.multiple_of(i * 256 + kx * 32, 32), 256)
            value = value + lax.dot_general(
                lhs_f[rows, :], mat_at[kx * 128 : kx * 128 + 128, :], along, preferred_element_type=F32
            )
        grad_input[pl.ds(pl.multiple_of(i * 256, 256), 256), :] = value.astype(BF16)
        return 0

    lax.fori_loop(0, 4, back_a, 0)
    sum_b.gather()
    sum_a.gather()

    fifteen_out = features.at[0:480]
    pltpu.make_async_copy(fifteen_out, fifteen_out, slab_sems.at[3]).wait()
    sum_b.finish()
    dwb[...] = out_b[0:1728, :].astype(F32) * scale_b
    dbb[...] = out_b[1728:1744, :].astype(F32)[0:1] * scale_b
    sum_a.finish()
    for k in range(27):
        row = k % 14 * 32
        value = out_a[row : row + 32, :].astype(F32) * scale_a
        if k >= 14:
            value = pltpu.roll(value, 64, 1)
        dwa[k * 32 : k * 32 + 32, :] = value[:, :64]
    dba[...] = out_a[448:464, :].astype(F32)[0:1, :64] * scale_a

    for sem, ref in ((0, land_v), (2, land_p), (4, land_g), (6, land_f)):
        pltpu.make_async_copy(ref, ref, halo_sems.at[sem]).wait()
    pltpu.make_async_copy(fifteen, fifteen, slab_sems.at[0]).wait()
    pltpu.make_async_copy(fifteen, fifteen, slab_sems.at[2]).wait()
    sum_b.drain()
    sum_a.drain()


def on_device(volume, weight_a, bias_a, weight_b, bias_b, cotangent):
    cells = 64 * 64 * 256
    scale_a, scale_b = 1.0 / math.sqrt(cells), 1.0 / math.sqrt(cells // 8)
    rows = volume.reshape(32, 32, 4, 2, 8, 2).transpose(1, 2, 4, 3, 5, 0).reshape(1024, 128)
    cot = cotangent.reshape(128, 4, 16, 8).transpose(2, 1, 3, 0).reshape(512, 128)

    def vm(shape, dtype):
        return pltpu.VMEM(shape, dtype)

    hv, hc, hf = HALO_VOLUME, HALO_COARSE, HALO_GRAD_A
    fine_rows, coarse_rows = 34 * 6 * PITCH, 18 * 6 * PITCH
    scratch = [
        vm((fine_rows, 128), F32), vm((coarse_rows, 128), F32), vm((coarse_rows, 128), F32),
        vm((fine_rows, 128), F32), vm((fine_rows, 128), F32),
        vm((1088, 512), BF16), vm((576, 640), BF16), vm((576, 1152), BF16), vm((1088, 1024), BF16),
        vm((1152, 128), BF16), vm((1536, 256), BF16), vm((1920, 128), BF16), vm((384, 1152), BF16),
        vm((384, 1024), BF16),
        vm((1024, 256), F32), vm((512, 128), BF16), vm((512, 128), BF16), vm((512, 128), BF16),
        vm((1024, 256), BF16), vm((1536, 256), F32),
        vm((hv.stage_rows, 128), BF16), vm((hv.rows, 128), BF16),
        vm((hc.stage_rows, 128), BF16), vm((hc.rows, 128), BF16),
        vm((hc.stage_rows, 128), BF16), vm((hc.rows, 128), BF16),
        vm((hf.stage_rows, 128), BF16), vm((hf.rows, 128), BF16),
    ]
    for chunk in (CHUNK_A, CHUNK_B):
        for count in (GROUP, GROUP - 1, 8, GROUP):
            scratch.append(vm((count * chunk, 128), BF16))
    scratch += [pltpu.SemaphoreType.DMA((k,)) for k in (8, 4, 6, 6)]
    outs = [
        jax.ShapeDtypeStruct((512, 128), BF16),
        jax.ShapeDtypeStruct((1024, 128), BF16),
        jax.ShapeDtypeStruct((864, 64), F32),
        jax.ShapeDtypeStruct((1, 64), F32),
        jax.ShapeDtypeStruct((1728, 128), F32),
        jax.ShapeDtypeStruct((1, 128), F32),
    ]
    space = pl.BlockSpec(memory_space=pltpu.VMEM)
    features, grad_input, dwa, dba, dwb, dbb = pl.pallas_call(
        lambda *refs: kernel(scale_a, scale_b, *refs),
        name="window",
        out_shape=outs,
        in_specs=[space] * 6,
        out_specs=[space] * 6,
        scratch_shapes=scratch,
        compiler_params=pltpu.CompilerParams(collective_id=0, has_side_effects=True),
    )(
        rows,
        weight_a.reshape(27, 32, 64),
        bias_a.reshape(1, 64),
        weight_b.reshape(27, 64, 128),
        bias_b.reshape(1, 128),
        cot,
    )
    features = features.reshape(16, 4, 8, 128).transpose(3, 1, 0, 2).reshape(128, 1, 4, 128)
    grad_input = grad_input.reshape(32, 4, 8, 2, 2, 32).transpose(5, 0, 1, 3, 2, 4).reshape(32, 32, 8, 16)
    return (
        features,
        grad_input,
        dwa.reshape(3, 3, 3, 32, 64),
        dba.reshape(64),
        dwb.reshape(3, 3, 3, 64, 128),
        dbb.reshape(128),
    )


def solution(mesh):
    return jax.shard_map(
        on_device,
        mesh=mesh,
        in_specs=(P(None, "gx", "gy", "gz"), P(), P(), P(), P(), P(None, ("gx", "gz"), "gy", None)),
        out_specs=(P(None, ("gx", "gz"), "gy", None), P(None, "gx", "gy", "gz"), P(), P(), P(), P()),
        check_vma=False,
    )
```
